512 devices in a mesh: row: 16 (over y_lo, x, core), col: 32 (over z, y_hi).
Axes of the slice: x: 4, y: 4 (y_hi: 2, y_lo: 2; y = y_hi * 2 + y_lo), z: 16, core: 2. Of those that a mesh axis runs over, the one named last changes fastest.
Arguments:
- users: bfloat16 [524288, 256], P(('row', 'col')), may hold values from -20 to 20
- positives: int32 [524288], P(('row', 'col')), may hold values from 0 to 8191
- items: bfloat16 [8192, 256], P(('row', 'col')), may hold values from -6 to 6
- item_ids: int32 [8192], P(('row', 'col')), may hold values from 0 to 999999
Outputs:
- loss: float32 [524288], P(('row', 'col'))
The draws below stay inside these ranges and needn't reach their ends.
All inputs are finite; a program needn't handle non-finite values.
Results may differ from the reference program's by a relative error of at most 0.0003.
Values may be sent and summed in bfloat16 or wider, within the bound.
A program may use at most 128 MiB of HBM per device.

```python
import math
import jax
import jax.numpy as jnp
import numpy as np
from jax import lax

E = 256
ITEMS_DEV = 16
USERS = 524288
ITEMS = 8192


def drawn(key):
    item_key = jax.random.fold_in(key, 11)
    user_key = jax.random.fold_in(key, 12)
    items = jnp.clip(jax.random.normal(item_key, (ITEMS, E), jnp.float32), -6.0, 6.0)
    users = jnp.clip(jax.random.normal(user_key, (USERS, E), jnp.float32), -6.0, 6.0)
    return (users, items)


def draw_users(key, part):
    return drawn(key)[0].astype(jnp.bfloat16)


def draw_items(key, part):
    return drawn(key)[1].astype(jnp.bfloat16)


def place_ends(drawn, own_key, low, high):
    spot = [jax.random.randint(jax.random.fold_in(own_key, axis), (), 0, length) for axis, length in enumerate(drawn.shape)]
    widest = drawn.shape.index(max(drawn.shape))
    neighbour = spot[:widest] + [(spot[widest] + 1) % drawn.shape[widest]] + spot[widest + 1:]
    return drawn.at[tuple(spot)].set(low).at[tuple(neighbour)].set(high)


def wide_ids(rng, shape, count, lean):
    portions = [min(1 << octave, count + 1 - (1 << octave)) * (1 << 20) // math.isqrt((1 << octave) ** lean) + 1 for octave in range((count + 1).bit_length()) if 1 << octave <= count]
    scale = 1 + sum(portions) // (1 << 30)
    listing = np.cumsum(np.array([max(1, weight // scale) for weight in portions]))
    ticket = jax.random.randint(jax.random.fold_in(rng, 1), shape, 0, int(listing[len(portions) - 1]))
    start = jnp.left_shift(1, jnp.searchsorted(jnp.asarray(listing, jnp.int32), ticket, side="right").astype(jnp.int32))
    rank = start - 1 + jax.random.randint(jax.random.fold_in(rng, 4), shape, 0, 1 << 30) % jnp.minimum(start, count + 1 - start)
    return jax.random.permutation(jax.random.fold_in(rng, 2), count)[rank].astype(jnp.int32)


def setup_inputs(seed: int = 0) -> dict:
    key_list = jax.random.split(jax.random.key(seed), 5)
    users = draw_users(jax.random.fold_in(key_list[4], 71), 0)
    positives = place_ends(jax.random.randint(key_list[1], (USERS,), 0, ITEMS), jax.random.fold_in(key_list[1], 1), 0, ITEMS - 1).astype(jnp.int32)
    items = draw_items(jax.random.fold_in(key_list[4], 71), 0)
    item_ids = place_ends(wide_ids(key_list[3], (ITEMS,), 1000000, 2), jax.random.fold_in(key_list[3], 3), 0, 999999).astype(jnp.int32)
    return {"users": users, "positives": positives, "items": items, "item_ids": item_ids}


def reference(users, positives, items, item_ids):
    pos_id = item_ids[positives]
    block = ITEMS_DEV * 8
    count = ITEMS // block
    init = (jnp.full((USERS,), -1e30, jnp.float32), jnp.zeros((USERS,), jnp.float32), jnp.zeros((USERS,), jnp.float32))

    def step(carry, index):
        high, summed, chosen = carry
        start = (index * block).astype(jnp.int32)
        piece = lax.dynamic_slice_in_dim(items, start, block, 0)
        ids = lax.dynamic_slice_in_dim(item_ids, start, block, 0)
        where_at = start + jnp.arange(block, dtype=jnp.int32)
        scores = 0.125 * jnp.dot(users, piece.T, preferred_element_type=jnp.float32)
        hit = where_at[None, :] == positives[:, None]
        keep = (ids[None, :] != pos_id[:, None]) | hit
        masked = jnp.where(keep, scores, -1e30)
        new_high = jnp.maximum(high, jnp.max(masked, axis=1))
        terms = jnp.where(keep, jnp.exp(masked - new_high[:, None]), 0.0)
        summed = summed * jnp.exp(high - new_high) + jnp.sum(terms, axis=1)
        chosen = chosen + jnp.sum(jnp.where(hit, scores, 0.0), axis=1)
        return (new_high, summed, chosen), None

    carry, _ = lax.scan(step, init, jnp.arange(count, dtype=jnp.int32))
    high, summed, chosen = carry
    return high + jnp.log(summed) - chosen
```

```python
import math

import jax
import jax.numpy as jnp
from jax import lax
from jax.experimental import pallas as pl
from jax.experimental.pallas import tpu as pltpu
from jax.sharding import PartitionSpec as P

SCALE = 0.125 * math.log2(math.e)
LN2 = math.log(2.0)
LOW = -1e30
START = -1e20
CHUNK = 256


def absorb_chunk(scores, id_row, base, pos_ref, pid_ref, iota_ref, high_ref, sum_ref, hit_ref):
    users = scores.shape[1]
    for half in range(CHUNK // 128):
        ids = jnp.broadcast_to(id_row[:, half * 128 : (half + 1) * 128], (128, 128)).T
        for group in range(users // 128):
            lanes = pl.ds(group * 128, 128)
            pos = pos_ref[:, lanes] - (base + half * 128)
            pid = pid_ref[:, lanes]
            chosen = hit_ref[:, lanes]
            high = high_ref[:, lanes]
            terms = []
            for k in range(16):
                d = scores[pl.ds(half * 128 + k * 8, 8), lanes]
                chosen = jnp.where(iota_ref[pl.ds(k * 8, 8), :] == pos, d, chosen)
                terms.append(jnp.where(ids[k * 8 : k * 8 + 8] == pid, LOW, d * SCALE))
            tops = terms
            while len(tops) > 1:
                tops = [jnp.maximum(a, b) for a, b in zip(tops[::2], tops[1::2])]
            new_high = jnp.maximum(high, tops[0])
            parts = [jnp.exp2(t - new_high) for t in terms]
            while len(parts) > 1:
                parts = [a + b for a, b in zip(parts[::2], parts[1::2])]
            sum_ref[:, lanes] = sum_ref[:, lanes] * jnp.exp2(high - new_high) + parts[0]
            high_ref[:, lanes] = new_high
            hit_ref[:, lanes] = chosen


def look_up(table, pos):
    low, hi = pos & 255, pos >> 8
    count = pos.shape[1]
    one_hot = jnp.where(lax.broadcasted_iota(jnp.int32, (256, count), 0) == low, 1.0, 0.0).astype(jnp.bfloat16)
    pieces = jnp.concatenate([table & 127, (table >> 7) & 127, table >> 14], axis=0)
    found = jnp.dot(pieces.astype(jnp.float32).astype(jnp.bfloat16), one_hot, preferred_element_type=jnp.float32)
    value = found[:32] + 128.0 * found[32:64] + 16384.0 * found[64:]
    mine = lax.broadcasted_iota(jnp.int32, (32, count), 0) == hi
    return jnp.sum(jnp.where(mine, value, 0.0), axis=0, keepdims=True)


def kernel(users_ref, pos_in, items_ref, table_ref, out_ref, ut_ref, s0, s1, pos_ref, pid_ref, iota_ref, high_ref, sum_ref, hit_ref, idf_ref):
    count = users_ref.shape[0]
    chunks = items_ref.shape[0] // CHUNK
    for i in range(count // 256):
        ut_ref[:, pl.ds(i * 256, 256)] = users_ref[pl.ds(i * 256, 256), :].T
    pos = pos_in[...]
    pos_ref[...] = jnp.broadcast_to(pos, pos_ref.shape)
    pid_ref[...] = jnp.broadcast_to(look_up(table_ref[...], pos), pid_ref.shape)
    idf_ref[...] = table_ref[...].astype(jnp.float32)
    iota_ref[...] = lax.broadcasted_iota(jnp.int32, (128, 128), 0)
    high_ref[...] = jnp.full_like(high_ref, START)
    sum_ref[...] = jnp.zeros_like(sum_ref)
    hit_ref[...] = jnp.zeros_like(hit_ref)

    def score(into, chunk):
        rows = pl.ds(pl.multiple_of(chunk * CHUNK, CHUNK), CHUNK)
        for i in range(count // 256):
            cols = pl.ds(i * 256, 256)
            into[:, cols] = jnp.dot(items_ref[rows, :], ut_ref[:, cols], preferred_element_type=jnp.float32)

    def absorb(scores, chunk):
        absorb_chunk(scores, idf_ref[pl.ds(chunk, 1), :], chunk * CHUNK, pos_ref, pid_ref, iota_ref, high_ref, sum_ref, hit_ref)

    score(s0, 0)

    def step(i, _):
        score(s1, 2 * i + 1)
        absorb(s0, 2 * i)
        score(s0, jnp.minimum(2 * i + 2, chunks - 1))
        absorb(s1, 2 * i + 1)
        return 0

    lax.fori_loop(0, chunks // 2, step, 0)
    chosen = jnp.sum(hit_ref[...], axis=0, keepdims=True)
    own = chosen * SCALE
    high = high_ref[...]
    top = jnp.maximum(jnp.max(high, axis=0, keepdims=True), own)
    total = jnp.sum(sum_ref[...] * jnp.exp2(high - top), axis=0, keepdims=True) + jnp.exp2(own - top)
    out_ref[...] = (top - own) * LN2 + jnp.log(total)


def body(users, positives, items, item_ids):
    table = lax.all_gather(item_ids, ("row", "col"), axis=0, tiled=True)
    pool = lax.all_gather(items, ("row", "col"), axis=0, tiled=True)
    count = users.shape[0]
    vmem = pl.BlockSpec(memory_space=pltpu.VMEM)
    state = pltpu.VMEM((8, count), jnp.float32)
    loss = pl.pallas_call(
        kernel,
        out_shape=jax.ShapeDtypeStruct((1, count), jnp.float32),
        in_specs=[vmem] * 4,
        out_specs=vmem,
        scratch_shapes=[
            pltpu.VMEM((256, count), jnp.bfloat16),
            pltpu.VMEM((CHUNK, count), jnp.float32),
            pltpu.VMEM((CHUNK, count), jnp.float32),
            pltpu.VMEM((8, count), jnp.int32),
            state,
            pltpu.VMEM((128, 128), jnp.int32),
            state,
            state,
            state,
            pltpu.VMEM((32, 256), jnp.float32),
        ],
        compiler_params=pltpu.CompilerParams(vmem_limit_bytes=32 * 1024 * 1024),
    )(users, positives.reshape(1, count), pool, table.reshape(32, 256))
    return loss.reshape(count)


def solution(mesh):
    split = P(("row", "col"))
    wide = P(("row", "col"), None)
    return jax.shard_map(body, mesh=mesh, in_specs=(wide, split, wide, split), out_specs=split, check_vma=False)
```

```python
import math

import jax
import jax.numpy as jnp
from jax import lax
from jax.experimental import pallas as pl
from jax.experimental.pallas import tpu as pltpu
from jax.sharding import PartitionSpec as P

MESH = pl.DeviceIdType.MESH
SCALE = 0.125 * math.log2(math.e)
LN2 = math.log(2.0)
LOW = -1e30
START = -1e20
SMALL = 2.0**-80
LARGE = 2.0**100
LAG = 3
NEAR = (4, 12, 1, 15, 2, 14, 3, 13)
FAR = (8, 9, 7, 10, 6, 11, 5)
PAIRS = ((0,), (1, 15), (2, 14), (3, 13), (4, 12), (5, 11), (6, 10), (7, 9), (8,))
IDS_AT = 5
MASK_AT = 10


def place():
    row, col = lax.axis_index("row"), lax.axis_index("col")
    return (row // 2) % 4, (col % 2) * 2 + row // 8, col // 2, row % 2


def device(x, y, z, c):
    return ((y % 2) * 4 + x) * 2 + c, z * 2 + y // 2


def id_columns(table, core):
    halves = []
    for half in range(2):
        rows = table[pl.ds(core * 16, 16), half, :]
        square = jnp.concatenate([rows, jnp.zeros((112, 128), jnp.float32)], axis=0)
        halves.append(square.T)
    return jnp.concatenate(halves, axis=0)


def fill_ids(into, columns, z_from, x_first):
    rows = columns[pl.ds(pl.multiple_of(z_from * 16, 16), 16), :]
    for block in range(16):
        lane = (block % 4) * 4 + block // 4 if x_first else block
        into[pl.ds(block * 16, 16), :] = jnp.broadcast_to(rows[:, lane : lane + 1], (16, 128))


def look_up(table, low, high):
    count = low.shape[1]
    found = None
    for half in range(2):
        ints = table[:, half, :].astype(jnp.int32)
        pieces = jnp.concatenate([ints & 127, (ints >> 7) & 127, ints >> 14], axis=0)
        pieces = pieces.astype(jnp.float32).astype(jnp.bfloat16)
        lanes = lax.broadcasted_iota(jnp.int32, (128, count), 0) + half * 128
        one_hot = jnp.where(lanes == low, 1.0, 0.0).astype(jnp.bfloat16)
        part = jnp.dot(pieces, one_hot, preferred_element_type=jnp.float32)
        found = part if found is None else found + part
    value = found[:32] + 128.0 * found[32:64] + 16384.0 * found[64:]
    mine = lax.broadcasted_iota(jnp.int32, (32, count), 0) == high
    return jnp.sum(jnp.where(mine, value, 0.0), axis=0, keepdims=True)


def split(pos):
    row, col = pos >> 9, (pos >> 4) & 31
    return (row >> 1) & 3, (col & 1) * 2 + (row >> 3), col >> 1, row & 1, pos & 15


def gather_kernel(
    users_hbm, pos_hbm, items_hbm, ids_hbm,
    stat_ref, table_ref, pool_hbm,
    grid, users, pos, ids_in, ids_z, ids_own, ut, prob, key_ref, pid_ref, iota_ref, hit_ref, acc_ref, cols_ref, idc_ref, mine_ref, theirs_ref,
    lsem, s1, r1, s2, r2, s3, r3, si, ri, st, rt, su, ru, se, re, le, sf, rf,
):
    x, y, z, c = place()

    def at(dx, dy, dz):
        return device((x + dx) % 4, (y + dy) % 4, (z + dz) % 16, c)

    partner = device(x, y, z, 1 - c)

    def send(src, dst, out_sem, in_sem, to):
        return pltpu.make_async_remote_copy(src, dst, out_sem, in_sem, device_id=to, device_id_type=MESH)

    barrier = pltpu.get_barrier_semaphore()
    loads = [
        pltpu.make_async_copy(items_hbm, grid.at[0, y, x], lsem.at[0]),
        pltpu.make_async_copy(ids_hbm, ids_in, lsem.at[1]),
        pltpu.make_async_copy(users_hbm, users.at[c], lsem.at[2]),
        pltpu.make_async_copy(pos_hbm, pos.at[c], lsem.at[3]),
    ]
    for load in loads:
        load.start()
    across = [(dx, dy, dc) for dx in range(4) for dy in range(4) for dc in range(2) if (dx, dy, dc) != (0, 0, 0)]

    def other(dx, dy, dc):
        return device((x + dx) % 4, (y + dy) % 4, z, (c + dc) % 2)

    for s in NEAR:
        pl.semaphore_signal(barrier, inc=1, device_id=at(0, 0, s), device_id_type=MESH)
    for to in across:
        pl.semaphore_signal(barrier, inc=1, device_id=other(*to), device_id_type=MESH)
    iota_ref[...] = lax.broadcasted_iota(jnp.int32, (256, 128), 0)
    hit_ref[...] = jnp.zeros_like(hit_ref)
    acc_ref[...] = jnp.zeros_like(acc_ref)
    for load in loads:
        load.wait()
    spread = jnp.concatenate([ids_in[...]] * 8, axis=1).astype(jnp.float32)
    lane = lax.broadcasted_iota(jnp.int32, (1, 128), 1)
    ids_z[0] = jnp.where(lane // 16 == z % 8, spread, 0.0)
    pl.semaphore_wait(barrier, len(NEAR) + len(across))

    def slot(s):
        return (s, y, x) if s < 8 else (s, x, y)

    def ids_copy(s):
        via = 0 if s in NEAR else (4 if s < 9 else 12)
        return send(ids_z.at[via], ids_z.at[s], si.at[s], ri.at[s], at(0, 0, s - via))

    def stage1(s):
        via = 0 if s in NEAR else (4 if s < 9 else 12)
        src = grid.at[slot(via)]
        return send(src, grid.at[slot(s)], s1.at[s], r1.at[s], at(0, 0, s - via))

    def stage2(s, d):
        block = grid.at[slot(s)]
        return send(block, block, s2.at[s, d], r2.at[s, d], at(d, 0, 0) if s < 8 else at(0, d, 0))

    def stage3(s, d):
        blocks = grid.at[slot(s)[:2]]
        return send(blocks, blocks, s3.at[s, d], r3.at[s, d], at(0, d, 0) if s < 8 else at(d, 0, 0))

    def export(s):
        return send(grid.at[s], pool_hbm.at[c, s], se.at[s], re.at[s], partner)

    def export_here(s):
        return pltpu.make_async_copy(grid.at[s], pool_hbm.at[c, s], le.at[s])

    own_row = c * 16 + y * 4 + x

    def table_copy(n, dx, dy, dc):
        dst = table_ref.at[own_row]
        return send(ids_own, dst, st.at[n], rt.at[n], other(dx, dy, dc))

    swaps = [
        send(users.at[c], users.at[c], su.at[0], ru.at[0], partner),
        send(pos.at[c], pos.at[c], su.at[1], ru.at[1], partner),
    ]
    for s in NEAR:
        ids_copy(s).start()
        stage1(s).start()
    for swap in swaps:
        swap.start()

    def turn_users():
        for swap in swaps:
            swap.wait_recv()
        for half in range(2):
            for i in range(4):
                ut[:, pl.ds(half * 1024 + i * 256, 256)] = users[half, pl.ds(i * 256, 256), :].T
        for half in range(2):
            px, py, pz, pc, pe = split(pos[half])
            s = (z - pz + 16) & 15
            block = jnp.where(s < 8, py * 4 + px, px * 4 + py)
            key_ref[half] = jnp.where(pc == c, s * 256 + block * 16 + pe, -1)

    def share_ids():
        for s in (1, 2, 3, 13, 14, 15) + FAR:
            ids_copy(s).wait_recv()
        rows = ids_z[:, 0, :]
        source = (z - lax.broadcasted_iota(jnp.int32, (16, 128), 0) + 16) & 15
        for half in range(2):
            mine = jnp.sum(jnp.where(source // 8 == half, rows, 0.0), axis=0, keepdims=True)
            ids_own[pl.ds(half, 1), :] = mine
        table_ref[own_row] = ids_own[...]
        for n, to in enumerate(across):
            table_copy(n, *to).start()

    def find_ids():
        for n, to in enumerate(across):
            table_copy(n, *to).wait_recv()
        for half in range(2):
            for g in range(8):
                px, py, pz, pc, pe = split(pos[half, pl.ds(g, 1), :])
                pid_ref[half, pl.ds(g, 1), :] = look_up(table_ref, pz * 16 + pe, pc * 16 + py * 4 + px)
        cols_ref[...] = id_columns(table_ref, c)

    def evaluate(s):
        block = grid[s].reshape(256, 256)
        for tile in range(8):
            d = jnp.dot(block, ut[:, pl.ds(tile * 256, 256)], preferred_element_type=jnp.float32)
            prob[s, :, pl.ds(tile * 256, 256)] = jnp.exp2(d * SCALE)
            for part in range(2):
                g = tile * 2 + part
                want = jnp.broadcast_to(key_ref[g // 8, pl.ds(g % 8, 1), :] - s * 256, (8, 128))
                chosen = hit_ref[:, pl.ds(g * 128, 128)]
                for k in range(32):
                    here = d[k * 8 : k * 8 + 8, part * 128 : part * 128 + 128]
                    chosen = jnp.where(iota_ref[pl.ds(k * 8, 8), :] == want, here, chosen)
                hit_ref[:, pl.ds(g * 128, 128)] = chosen

    def collect(s):
        fill_ids(idc_ref, cols_ref, (z - s + 16) & 15, s >= 8)
        for g in range(16):
            pid = jnp.broadcast_to(pid_ref[g // 8, pl.ds(g % 8, 1), :], (8, 128))
            sums = [acc_ref[:, pl.ds(g * 128, 128)], None, None, None]
            for k in range(32):
                rows = pl.ds(k * 8, 8)
                term = jnp.where(idc_ref[rows, :] == pid, 0.0, prob[s, rows, pl.ds(g * 128, 128)])
                sums[k % 4] = term if sums[k % 4] is None else sums[k % 4] + term
            acc_ref[:, pl.ds(g * 128, 128)] = (sums[0] + sums[1]) + (sums[2] + sums[3])

    done = []
    count = len(PAIRS)
    for t in range(count + 2 * LAG):
        if t < count:
            if t == 3:
                for s in (4, 12):
                    ids_copy(s).wait_recv()
                    stage1(s).wait_recv()
                for s in FAR:
                    ids_copy(s).start()
                    stage1(s).start()
            for s in PAIRS[t]:
                if s not in (0, 4, 12):
                    stage1(s).wait_recv()
                for d in (1, 3, 2):
                    stage2(s, d).start()
        if 0 <= t - LAG < count:
            for s in PAIRS[t - LAG]:
                for d in (1, 3, 2):
                    stage2(s, d).wait_recv()
                for d in (1, 3, 2):
                    stage3(s, d).start()
        if t == 1:
            turn_users()
        if t == IDS_AT:
            share_ids()
        if t == MASK_AT:
            find_ids()
        if t - 2 * LAG >= 0:
            for s in PAIRS[t - 2 * LAG]:
                for d in (1, 3, 2):
                    stage3(s, d).wait_recv()
                export(s).start()
                export_here(s).start()
                evaluate(s)
                done.append(s)
        if t >= MASK_AT:
            for s in done:
                collect(s)
            done = []

    for half in range(2):
        for g in range(8):
            lanes = pl.ds((half * 8 + g) * 128, 128)
            mine_ref[half, 0, pl.ds(g, 1), :] = jnp.sum(acc_ref[:, lanes], axis=0, keepdims=True)
            mine_ref[half, 1, pl.ds(g, 1), :] = jnp.sum(hit_ref[:, lanes], axis=0, keepdims=True)
    last = send(mine_ref.at[1 - c], theirs_ref, sf, rf, partner)
    last.start()
    for swap in swaps:
        swap.wait_send()
    for s in NEAR + FAR:
        ids_copy(s).wait_send()
        stage1(s).wait_send()
    for s in range(16):
        for d in (1, 2, 3):
            stage2(s, d).wait_send()
            stage3(s, d).wait_send()
        export(s).wait()
        export_here(s).wait()
    for n, to in enumerate(across):
        table_copy(n, *to).wait_send()
    last.wait()
    chosen = mine_ref[c, 1] + theirs_ref[1]
    total = mine_ref[c, 0] + theirs_ref[0] + jnp.exp2(chosen * SCALE)
    stat_ref[0] = jnp.log(total) - 0.125 * chosen
    stat_ref[1] = total
    stat_ref[2] = chosen
    stat_ref[3] = pid_ref[c]


def finish_kernel(stat_ref, table_hbm, users_hbm, pool_hbm, out_ref, table, users, ut, block, cols, idc, high_ref, sum_ref, sem):
    total = stat_ref[1]
    out_ref[...] = stat_ref[0]
    fine = jnp.where((total > SMALL) & (total < LARGE), 0.0, 1.0)

    @pl.when(jnp.max(fine) > 0.0)
    def _():
        z = lax.axis_index("col") // 2
        for src, dst in ((table_hbm, table), (users_hbm, users)):
            copy = pltpu.make_async_copy(src, dst, sem)
            copy.start()
            copy.wait()
        for i in range(4):
            ut[:, pl.ds(i * 256, 256)] = users[pl.ds(i * 256, 256), :].T
        high_ref[...] = jnp.full_like(high_ref, START)
        sum_ref[...] = jnp.zeros_like(sum_ref)
        for core in range(2):
            cols[...] = id_columns(table, core)

            def absorb(s, x_first):
                copy = pltpu.make_async_copy(pool_hbm.at[core, s], block, sem)
                copy.start()
                copy.wait()
                fill_ids(idc, cols, (z - s + 16) & 15, x_first)
                for g in range(8):
                    lanes = pl.ds(g * 128, 128)
                    d = jnp.dot(block[...].reshape(256, 256), ut[:, lanes], preferred_element_type=jnp.float32)
                    masked = jnp.where(idc[...] == stat_ref[3, pl.ds(g, 1), :], LOW, d * SCALE)
                    high = high_ref[pl.ds(g, 1), :]
                    top = jnp.maximum(high, jnp.max(masked, axis=0, keepdims=True))
                    part = jnp.sum(jnp.exp2(masked - top), axis=0, keepdims=True)
                    sum_ref[pl.ds(g, 1), :] = sum_ref[pl.ds(g, 1), :] * jnp.exp2(high - top) + part
                    high_ref[pl.ds(g, 1), :] = top

            lax.fori_loop(0, 8, lambda s, _: (absorb(s, False), 0)[1], 0)
            lax.fori_loop(8, 16, lambda s, _: (absorb(s, True), 0)[1], 0)
        own = stat_ref[2] * SCALE
        high = high_ref[...]
        top = jnp.maximum(high, own)
        both = sum_ref[...] * jnp.exp2(high - top) + jnp.exp2(own - top)
        out_ref[...] = (top - own) * LN2 + jnp.log(both)


def body(users, positives, items, item_ids):
    hbm = pl.BlockSpec(memory_space=pltpu.HBM)
    vmem = pl.BlockSpec(memory_space=pltpu.VMEM)
    f32, bf16, i32 = jnp.float32, jnp.bfloat16, jnp.int32
    dma = pltpu.SemaphoreType.DMA
    stat, table, pool = pl.pallas_call(
        gather_kernel,
        name="gather_scores",
        out_shape=(
            jax.ShapeDtypeStruct((4, 8, 128), f32),
            jax.ShapeDtypeStruct((32, 2, 128), f32),
            jax.ShapeDtypeStruct((2, 16, 4, 4, 16, 256), bf16),
        ),
        in_specs=[hbm] * 4,
        out_specs=(vmem, vmem, hbm),
        scratch_shapes=[
            pltpu.VMEM((16, 4, 4, 16, 256), bf16),
            pltpu.VMEM((2, 1024, 256), bf16),
            pltpu.VMEM((2, 8, 128), i32),
            pltpu.VMEM((1, 16), i32),
            pltpu.VMEM((16, 1, 128), f32),
            pltpu.VMEM((2, 128), f32),
            pltpu.VMEM((256, 2048), bf16),
            pltpu.VMEM((16, 256, 2048), f32),
            pltpu.VMEM((2, 8, 128), i32),
            pltpu.VMEM((2, 8, 128), f32),
            pltpu.VMEM((256, 128), i32),
            pltpu.VMEM((8, 2048), f32),
            pltpu.VMEM((8, 2048), f32),
            pltpu.VMEM((256, 128), f32),
            pltpu.VMEM((256, 128), f32),
            pltpu.VMEM((2, 2, 8, 128), f32),
            pltpu.VMEM((2, 8, 128), f32),
            dma((4,)),
            dma((16,)), dma((16,)),
            dma((16, 4)), dma((16, 4)),
            dma((16, 4)), dma((16, 4)),
            dma((16,)), dma((16,)),
            dma((31,)), dma((31,)),
            dma((2,)), dma((2,)),
            dma((16,)), dma((16,)), dma((16,)),
            dma, dma,
        ],
        compiler_params=pltpu.CompilerParams(collective_id=0, has_side_effects=True, vmem_limit_bytes=67_000_000),
    )(users, positives.reshape(8, 128), items, item_ids.reshape(1, 16))
    loss = pl.pallas_call(
        finish_kernel,
        name="finish",
        out_shape=jax.ShapeDtypeStruct((8, 128), f32),
        in_specs=[vmem, hbm, hbm, hbm],
        out_specs=vmem,
        scratch_shapes=[
            pltpu.VMEM((32, 2, 128), f32),
            pltpu.VMEM((1024, 256), bf16),
            pltpu.VMEM((256, 1024), bf16),
            pltpu.VMEM((4, 4, 16, 256), bf16),
            pltpu.VMEM((256, 128), f32),
            pltpu.VMEM((256, 128), f32),
            pltpu.VMEM((8, 128), f32),
            pltpu.VMEM((8, 128), f32),
            dma,
        ],
        compiler_params=pltpu.CompilerParams(vmem_limit_bytes=67_000_000),
    )(stat, table, users, pool)
    return loss.reshape(1024)


def solution(mesh):
    split_all = P(("row", "col"))
    wide = P(("row", "col"), None)
    return jax.shard_map(body, mesh=mesh, in_specs=(wide, split_all, wide, split_all), out_specs=split_all, check_vma=False)
```

```python
import math

import jax
import jax.numpy as jnp
from jax import lax
from jax.experimental import pallas as pl
from jax.experimental.pallas import tpu as pltpu
from jax.sharding import PartitionSpec as P

MESH = pl.DeviceIdType.MESH
SCALE = 0.125 * math.log2(math.e)
LN2 = math.log(2.0)
LOW = -1e30
START = -1e20
SMALL = 2.0**-80
LARGE = 2.0**100
IDS_NEAR = (4, 12, 1, 15, 2, 14, 3, 13)
NEAR = (4, 12, 3, 13)
FAR = (8, 9, 7, 10, 6, 11, 5)
WHOLE = (1, 15, 2, 14)


def place():
    row, col = lax.axis_index("row"), lax.axis_index("col")
    return (row // 2) % 4, (col % 2) * 2 + row // 8, col // 2, row % 2


def device(x, y, z, c):
    return ((y % 2) * 4 + x) * 2 + c, z * 2 + y // 2


def id_columns(table, core, x_first):
    halves = []
    for half in range(2):
        if x_first:
            picks = [table[core * 16 + (n % 4) * 4 + n // 4, pl.ds(half, 1), :] for n in range(16)]
            rows = jnp.concatenate(picks, axis=0)
        else:
            rows = table[pl.ds(core * 16, 16), half, :]
        square = jnp.concatenate([rows, jnp.zeros((112, 128), jnp.float32)], axis=0)
        halves.append(square.T)
    return jnp.concatenate(halves, axis=0)


def turned(s):
    return jnp.where((s >= 8) & (s < 14), 1, 0)


def fill_ids(into, columns, z_from, order):
    rows = columns[order, pl.ds(pl.multiple_of(z_from * 16, 16), 16), :]
    for block in range(16):
        into[pl.ds(block * 16, 16), :] = jnp.broadcast_to(rows[:, block : block + 1], (16, 128))


def look_up(table, low, high):
    count = low.shape[1]
    found = None
    for half in range(2):
        ints = table[:, half, :].astype(jnp.int32)
        pieces = jnp.concatenate([ints & 127, (ints >> 7) & 127, ints >> 14], axis=0)
        pieces = pieces.astype(jnp.float32).astype(jnp.bfloat16)
        lanes = lax.broadcasted_iota(jnp.int32, (128, count), 0) + half * 128
        one_hot = jnp.where(lanes == low, 1.0, 0.0).astype(jnp.bfloat16)
        part = jnp.dot(pieces, one_hot, preferred_element_type=jnp.float32)
        found = part if found is None else found + part
    value = found[:32] + 128.0 * found[32:64] + 16384.0 * found[64:]
    mine = lax.broadcasted_iota(jnp.int32, (32, count), 0) == high
    return jnp.sum(jnp.where(mine, value, 0.0), axis=0, keepdims=True)


def split(pos):
    row, col = pos >> 9, (pos >> 4) & 31
    return (row >> 1) & 3, (col & 1) * 2 + (row >> 3), col >> 1, row & 1, pos & 15


def gather_kernel(
    users_hbm, pos_hbm, items_hbm, ids_hbm,
    stat_ref, table_ref, pool_hbm,
    grid, users, pos, ids_in, ids_z, ids_own, ut, prob, key_ref, pid_ref, iota_ref, hit_ref, acc_ref, cols_ref, idc_ref, mine_ref, theirs_ref,
    lsem, s1, r1, s2, r2, s3, r3, sw, rw, si, ri, st, rt, su, ru, se, re, le, sf, rf,
):
    x, y, z, c = place()

    def at(dx, dy, dz):
        return device((x + dx) % 4, (y + dy) % 4, (z + dz) % 16, c)

    partner = device(x, y, z, 1 - c)

    def send(src, dst, out_sem, in_sem, to):
        return pltpu.make_async_remote_copy(src, dst, out_sem, in_sem, device_id=to, device_id_type=MESH)

    barrier = pltpu.get_barrier_semaphore()
    loads = [
        pltpu.make_async_copy(items_hbm, grid.at[0, y, x], lsem.at[0]),
        pltpu.make_async_copy(ids_hbm, ids_in, lsem.at[1]),
        pltpu.make_async_copy(users_hbm, users.at[c], lsem.at[2]),
        pltpu.make_async_copy(pos_hbm, pos.at[c], lsem.at[3]),
    ]
    for load in loads:
        load.start()
    across = [(dx, dy, dc) for dx in range(4) for dy in range(4) for dc in range(2) if (dx, dy, dc) != (0, 0, 0)]

    def other(dx, dy, dc):
        return device((x + dx) % 4, (y + dy) % 4, z, (c + dc) % 2)

    for s in IDS_NEAR:
        pl.semaphore_signal(barrier, inc=1, device_id=at(0, 0, s), device_id_type=MESH)
    for to in across:
        pl.semaphore_signal(barrier, inc=1, device_id=other(*to), device_id_type=MESH)
    iota_ref[...] = lax.broadcasted_iota(jnp.int32, (256, 128), 0)
    hit_ref[...] = jnp.zeros_like(hit_ref)
    acc_ref[...] = jnp.zeros_like(acc_ref)
    for load in loads:
        load.wait()
    spread = jnp.concatenate([ids_in[...]] * 8, axis=1).astype(jnp.float32)
    lane = lax.broadcasted_iota(jnp.int32, (1, 128), 1)
    ids_z[0] = jnp.where(lane // 16 == z % 8, spread, 0.0)
    pl.semaphore_wait(barrier, len(IDS_NEAR) + len(across))

    def slot(s):
        return (s, x, y) if 8 <= s < 14 else (s, y, x)

    def ids_copy(s):
        via = 0 if s in IDS_NEAR else (4 if s < 9 else 12)
        return send(ids_z.at[via], ids_z.at[s], si.at[s], ri.at[s], at(0, 0, s - via))

    def stage1(s):
        via = 0 if s in NEAR else (4 if s < 9 else 12)
        src = grid.at[slot(via)]
        return send(src, grid.at[slot(s)], s1.at[s], r1.at[s], at(0, 0, s - via))

    def stage2(s, d):
        block = grid.at[slot(s)]
        return send(block, block, s2.at[s, d], r2.at[s, d], at(d, 0, 0) if s < 8 else at(0, d, 0))

    def stage3(s, d):
        blocks = grid.at[slot(s)[:2]]
        return send(blocks, blocks, s3.at[s, d], r3.at[s, d], at(0, d, 0) if s < 8 else at(d, 0, 0))

    def whole(s):
        return send(grid.at[0], grid.at[s], sw.at[s], rw.at[s], at(0, 0, s))

    def export(s):
        return send(grid.at[s], pool_hbm.at[c, s], se.at[s], re.at[s], partner)

    def export_here(s):
        return pltpu.make_async_copy(grid.at[s], pool_hbm.at[c, s], le.at[s])

    own_row = c * 16 + y * 4 + x

    def table_copy(n, dx, dy, dc):
        dst = table_ref.at[own_row]
        return send(ids_own, dst, st.at[n], rt.at[n], other(dx, dy, dc))

    swaps = [
        send(users.at[c], users.at[c], su.at[0], ru.at[0], partner),
        send(pos.at[c], pos.at[c], su.at[1], ru.at[1], partner),
    ]
    for s in NEAR:
        stage1(s).start()
    for d in (1, 3, 2):
        stage2(0, d).start()
    for s in IDS_NEAR:
        ids_copy(s).start()
    for swap in swaps:
        swap.start()

    def turn_users():
        for swap in swaps:
            swap.wait_recv()
        for half in range(2):
            for i in range(4):
                ut[:, pl.ds(half * 1024 + i * 256, 256)] = users[half, pl.ds(i * 256, 256), :].T
        for half in range(2):
            px, py, pz, pc, pe = split(pos[half])
            s = (z - pz + 16) & 15
            block = jnp.where(turned(s) == 0, py * 4 + px, px * 4 + py)
            key_ref[half] = jnp.where(pc == c, s * 256 + block * 16 + pe, -1)

    def share_ids():
        for s in (1, 2, 3, 13, 14, 15) + FAR:
            ids_copy(s).wait_recv()
        rows = ids_z[:, 0, :]
        source = (z - lax.broadcasted_iota(jnp.int32, (16, 128), 0) + 16) & 15
        for half in range(2):
            mine = jnp.sum(jnp.where(source // 8 == half, rows, 0.0), axis=0, keepdims=True)
            ids_own[pl.ds(half, 1), :] = mine
        table_ref[own_row] = ids_own[...]
        for n, to in enumerate(across):
            table_copy(n, *to).start()

    def find_ids():
        for n, to in enumerate(across):
            table_copy(n, *to).wait_recv()
        for half in range(2):
            for g in range(8):
                px, py, pz, pc, pe = split(pos[half, pl.ds(g, 1), :])
                pid_ref[half, pl.ds(g, 1), :] = look_up(table_ref, pz * 16 + pe, pc * 16 + py * 4 + px)
        for order in range(2):
            cols_ref[order] = id_columns(table_ref, c, order == 1)

    def evaluate(s):
        block = grid[s].reshape(256, 256)
        for tile in range(8):
            d = jnp.dot(block, ut[:, pl.ds(tile * 256, 256)], preferred_element_type=jnp.float32)
            prob[s, :, pl.ds(tile * 256, 256)] = jnp.exp2(d * SCALE)
            for part in range(2):
                g = tile * 2 + part
                want = jnp.broadcast_to(key_ref[g // 8, pl.ds(g % 8, 1), :] - s * 256, (8, 128))
                chosen = hit_ref[:, pl.ds(g * 128, 128)]
                for k in range(32):
                    here = d[k * 8 : k * 8 + 8, part * 128 : part * 128 + 128]
                    chosen = jnp.where(iota_ref[pl.ds(k * 8, 8), :] == want, here, chosen)
                hit_ref[:, pl.ds(g * 128, 128)] = chosen

    def collect(s):
        fill_ids(idc_ref, cols_ref, (z - s + 16) & 15, turned(s))
        for g in range(16):
            pid = jnp.broadcast_to(pid_ref[g // 8, pl.ds(g % 8, 1), :], (8, 128))
            sums = [acc_ref[:, pl.ds(g * 128, 128)], None, None, None]
            for k in range(32):
                rows = pl.ds(k * 8, 8)
                term = jnp.where(idc_ref[rows, :] == pid, 0.0, prob[s, rows, pl.ds(g * 128, 128)])
                sums[k % 4] = term if sums[k % 4] is None else sums[k % 4] + term
            acc_ref[:, pl.ds(g * 128, 128)] = (sums[0] + sums[1]) + (sums[2] + sums[3])

    def forward(slots):
        for s in slots:
            for d in (1, 3, 2):
                stage2(s, d).wait_recv()
            for d in (1, 3, 2):
                stage3(s, d).start()

    def landed(s):
        for d in (1, 3, 2):
            send(grid.at[s, 0], grid.at[s, 0], s3.at[s, d], r3.at[s, d], partner).wait_recv()

    def hand_on(s):
        export(s).start()
        export_here(s).start()

    def loop(count, slot_of, step):
        def turn(i, carry):
            step(slot_of(i))
            return carry

        lax.fori_loop(0, count, turn, 0)

    def early(s):
        landed(s)
        hand_on(s)
        evaluate(s)

    def late_whole(s):
        send(grid.at[s], grid.at[s], sw.at[s], rw.at[s], partner).wait_recv()
        hand_on(s)
        evaluate(s)
        collect(s)

    def late(s):
        early(s)
        collect(s)

    turn_users()
    forward((0,))
    for s in (4, 12):
        stage1(s).wait_recv()
        ids_copy(s).wait_recv()
    for s in FAR:
        ids_copy(s).start()
        stage1(s).start()
    for s in (4, 12):
        for d in (1, 3, 2):
            stage2(s, d).start()
    for s in (3, 13):
        stage1(s).wait_recv()
        for d in (1, 3, 2):
            stage2(s, d).start()
    landed(0)
    for s in WHOLE:
        whole(s).start()
    hand_on(0)
    evaluate(0)
    forward((4, 12, 3, 13))
    share_ids()
    for s in FAR:
        stage1(s).wait_recv()
        for d in (1, 3, 2):
            stage2(s, d).start()
    loop(2, lambda i: 4 + 8 * i, early)
    forward(FAR[:4])
    loop(2, lambda i: 3 + 10 * i, early)
    forward(FAR[4:])
    find_ids()
    loop(5, lambda i: jnp.where(i < 2, i * 4, jnp.where(i == 2, 12, 10 * i - 27)), collect)
    loop(4, lambda i: jnp.where(i % 2 == 0, 1 + i // 2, 15 - i // 2), late_whole)
    loop(7, lambda i: 8 + jnp.where(i % 2 == 1, (i + 1) // 2, -(i // 2)), late)

    for half in range(2):
        for g in range(8):
            lanes = pl.ds((half * 8 + g) * 128, 128)
            mine_ref[half, 0, pl.ds(g, 1), :] = jnp.sum(acc_ref[:, lanes], axis=0, keepdims=True)
            mine_ref[half, 1, pl.ds(g, 1), :] = jnp.sum(hit_ref[:, lanes], axis=0, keepdims=True)
    last = send(mine_ref.at[1 - c], theirs_ref, sf, rf, partner)
    last.start()
    for swap in swaps:
        swap.wait_send()
    for s in range(1, 16):
        ids_copy(s).wait_send()
    for s in WHOLE:
        whole(s).wait_send()
    for s in NEAR + FAR:
        stage1(s).wait_send()
    for s in (0,) + NEAR + FAR:
        for d in (1, 2, 3):
            stage2(s, d).wait_send()
            stage3(s, d).wait_send()
    for s in range(16):
        export(s).wait()
        export_here(s).wait()
    for n, to in enumerate(across):
        table_copy(n, *to).wait_send()
    last.wait()
    chosen = mine_ref[c, 1] + theirs_ref[1]
    others = mine_ref[c, 0] + theirs_ref[0]
    own = jnp.exp2(chosen * SCALE)
    total = others + own
    stat_ref[0] = jnp.where(others < own, jnp.log(1.0 + others / own), jnp.log(total) - 0.125 * chosen)
    stat_ref[1] = total
    stat_ref[2] = chosen
    stat_ref[3] = pid_ref[c]


def finish_kernel(stat_ref, table_hbm, users_hbm, pool_hbm, out_ref, table, users, ut, block, cols, idc, high_ref, sum_ref, sem):
    total = stat_ref[1]
    out_ref[...] = stat_ref[0]
    fine = jnp.where((total > SMALL) & (total < LARGE), 0.0, 1.0)

    @pl.when(jnp.max(fine) > 0.0)
    def _():
        z = lax.axis_index("col") // 2
        for src, dst in ((table_hbm, table), (users_hbm, users)):
            copy = pltpu.make_async_copy(src, dst, sem)
            copy.start()
            copy.wait()
        for i in range(4):
            ut[:, pl.ds(i * 256, 256)] = users[pl.ds(i * 256, 256), :].T
        high_ref[...] = jnp.full_like(high_ref, START)
        sum_ref[...] = jnp.zeros_like(sum_ref)
        for core in range(2):
            for order in range(2):
                cols[order] = id_columns(table, core, order == 1)

            def absorb(s, _):
                copy = pltpu.make_async_copy(pool_hbm.at[core, s], block, sem)
                copy.start()
                copy.wait()
                fill_ids(idc, cols, (z - s + 16) & 15, turned(s))
                for g in range(8):
                    lanes = pl.ds(g * 128, 128)
                    d = jnp.dot(block[...].reshape(256, 256), ut[:, lanes], preferred_element_type=jnp.float32)
                    masked = jnp.where(idc[...] == stat_ref[3, pl.ds(g, 1), :], LOW, d * SCALE)
                    high = high_ref[pl.ds(g, 1), :]
                    top = jnp.maximum(high, jnp.max(masked, axis=0, keepdims=True))
                    part = jnp.sum(jnp.exp2(masked - top), axis=0, keepdims=True)
                    sum_ref[pl.ds(g, 1), :] = sum_ref[pl.ds(g, 1), :] * jnp.exp2(high - top) + part
                    high_ref[pl.ds(g, 1), :] = top

                return 0

            lax.fori_loop(0, 16, absorb, 0)
        own = stat_ref[2] * SCALE
        high = high_ref[...]
        top = jnp.maximum(high, own)
        both = sum_ref[...] * jnp.exp2(high - top) + jnp.exp2(own - top)
        out_ref[...] = (top - own) * LN2 + jnp.log(both)


def body(users, positives, items, item_ids):
    hbm = pl.BlockSpec(memory_space=pltpu.HBM)
    vmem = pl.BlockSpec(memory_space=pltpu.VMEM)
    f32, bf16, i32 = jnp.float32, jnp.bfloat16, jnp.int32
    dma = pltpu.SemaphoreType.DMA
    stat, table, pool = pl.pallas_call(
        gather_kernel,
        name="gather_scores",
        out_shape=(
            jax.ShapeDtypeStruct((4, 8, 128), f32),
            jax.ShapeDtypeStruct((32, 2, 128), f32),
            jax.ShapeDtypeStruct((2, 16, 4, 4, 16, 256), bf16),
        ),
        in_specs=[hbm] * 4,
        out_specs=(vmem, vmem, hbm),
        scratch_shapes=[
            pltpu.VMEM((16, 4, 4, 16, 256), bf16),
            pltpu.VMEM((2, 1024, 256), bf16),
            pltpu.VMEM((2, 8, 128), i32),
            pltpu.VMEM((1, 16), i32),
            pltpu.VMEM((16, 1, 128), f32),
            pltpu.VMEM((2, 128), f32),
            pltpu.VMEM((256, 2048), bf16),
            pltpu.VMEM((16, 256, 2048), f32),
            pltpu.VMEM((2, 8, 128), i32),
            pltpu.VMEM((2, 8, 128), f32),
            pltpu.VMEM((256, 128), i32),
            pltpu.VMEM((8, 2048), f32),
            pltpu.VMEM((8, 2048), f32),
            pltpu.VMEM((2, 256, 128), f32),
            pltpu.VMEM((256, 128), f32),
            pltpu.VMEM((2, 2, 8, 128), f32),
            pltpu.VMEM((2, 8, 128), f32),
            dma((4,)),
            dma((16,)), dma((16,)),
            dma((16, 4)), dma((16, 4)),
            dma((16, 4)), dma((16, 4)),
            dma((16,)), dma((16,)),
            dma((16,)), dma((16,)),
            dma((31,)), dma((31,)),
            dma((2,)), dma((2,)),
            dma((16,)), dma((16,)), dma((16,)),
            dma, dma,
        ],
        compiler_params=pltpu.CompilerParams(collective_id=0, has_side_effects=True, vmem_limit_bytes=67_000_000),
    )(users, positives.reshape(8, 128), items, item_ids.reshape(1, 16))
    loss = pl.pallas_call(
        finish_kernel,
        name="finish",
        out_shape=jax.ShapeDtypeStruct((8, 128), f32),
        in_specs=[vmem, hbm, hbm, hbm],
        out_specs=vmem,
        scratch_shapes=[
            pltpu.VMEM((32, 2, 128), f32),
            pltpu.VMEM((1024, 256), bf16),
            pltpu.VMEM((256, 1024), bf16),
            pltpu.VMEM((4, 4, 16, 256), bf16),
            pltpu.VMEM((2, 256, 128), f32),
            pltpu.VMEM((256, 128), f32),
            pltpu.VMEM((8, 128), f32),
            pltpu.VMEM((8, 128), f32),
            dma,
        ],
        compiler_params=pltpu.CompilerParams(vmem_limit_bytes=67_000_000),
    )(stat, table, users, pool)
    return loss.reshape(1024)


def solution(mesh):
    split_all = P(("row", "col"))
    wide = P(("row", "col"), None)
    return jax.shard_map(body, mesh=mesh, in_specs=(wide, split_all, wide, split_all), out_specs=split_all, check_vma=False)
```

```python
import math

import jax
import jax.numpy as jnp
from jax import lax
from jax.experimental import pallas as pl
from jax.experimental.pallas import tpu as pltpu
from jax.sharding import PartitionSpec as P

MESH = pl.DeviceIdType.MESH
SCALE = 0.125 * math.log2(math.e)
LN2 = math.log(2.0)
LOW = -1e30
START = -1e20
SMALL = 2.0**-80
LARGE = 2.0**100
NEAR = (4, 12, 6, 10, 5, 11, 3, 13)
FAR = (8, 9, 7)
WHOLE = (1, 15, 2, 14)


def place():
    row, col = lax.axis_index("row"), lax.axis_index("col")
    return (row // 2) % 4, (col % 2) * 2 + row // 8, col // 2, row % 2


def device(x, y, z, c):
    return ((y % 2) * 4 + x) * 2 + c, z * 2 + y // 2


def id_columns(table, core, x_first):
    halves = []
    for half in range(2):
        if x_first:
            picks = [table[core * 16 + (n % 4) * 4 + n // 4, pl.ds(half, 1), :] for n in range(16)]
            rows = jnp.concatenate(picks, axis=0)
        else:
            rows = table[pl.ds(core * 16, 16), half, :]
        square = jnp.concatenate([rows, jnp.zeros((112, 128), jnp.float32)], axis=0)
        halves.append(square.T)
    return jnp.concatenate(halves, axis=0)


def turned(s):
    return jnp.where((s >= 8) & (s < 14), 1, 0)


def fill_ids(into, columns, z_from, order):
    rows = columns[order, pl.ds(pl.multiple_of(z_from * 16, 16), 16), :]
    for block in range(16):
        into[pl.ds(block * 16, 16), :] = jnp.broadcast_to(rows[:, block : block + 1], (16, 128))


def look_up(table, low, high):
    count = low.shape[1]
    found = None
    for half in range(2):
        ints = table[:, half, :].astype(jnp.int32)
        pieces = jnp.concatenate([ints & 127, (ints >> 7) & 127, ints >> 14], axis=0)
        pieces = pieces.astype(jnp.float32).astype(jnp.bfloat16)
        lanes = lax.broadcasted_iota(jnp.int32, (128, count), 0) + half * 128
        one_hot = jnp.where(lanes == low, 1.0, 0.0).astype(jnp.bfloat16)
        part = jnp.dot(pieces, one_hot, preferred_element_type=jnp.float32)
        found = part if found is None else found + part
    value = found[:32] + 128.0 * found[32:64] + 16384.0 * found[64:]
    mine = lax.broadcasted_iota(jnp.int32, (32, count), 0) == high
    return jnp.sum(jnp.where(mine, value, 0.0), axis=0, keepdims=True)


def split(pos):
    row, col = pos >> 9, (pos >> 4) & 31
    return (row >> 1) & 3, (col & 1) * 2 + (row >> 3), col >> 1, row & 1, pos & 15


def gather_kernel(
    users_hbm, pos_hbm, items_hbm, ids_hbm,
    stat_ref, table_ref, pool_hbm,
    grid, users, pos, ids_in, ids_z, ids_own, ut, prob, key_ref, pid_ref, iota_ref, hit_ref, acc_ref, cols_ref, idc_ref, mine_ref, theirs_ref,
    lsem, s1, r1, s2, r2, s3, r3, sw, rw, si, ri, st, rt, su, ru, se, re, le, sf, rf,
):
    x, y, z, c = place()

    def at(dx, dy, dz):
        return device((x + dx) % 4, (y + dy) % 4, (z + dz) % 16, c)

    partner = device(x, y, z, 1 - c)

    def send(src, dst, out_sem, in_sem, to):
        return pltpu.make_async_remote_copy(src, dst, out_sem, in_sem, device_id=to, device_id_type=MESH)

    barrier = pltpu.get_barrier_semaphore()
    loads = [
        pltpu.make_async_copy(items_hbm, grid.at[0, y, x], lsem.at[0]),
        pltpu.make_async_copy(ids_hbm, ids_in, lsem.at[1]),
        pltpu.make_async_copy(users_hbm, users.at[c], lsem.at[2]),
        pltpu.make_async_copy(pos_hbm, pos.at[c], lsem.at[3]),
    ]
    for load in loads:
        load.start()
    across = [(dx, dy, dc) for dx in range(4) for dy in range(4) for dc in range(2) if (dx, dy, dc) != (0, 0, 0)]

    def other(dx, dy, dc):
        return device((x + dx) % 4, (y + dy) % 4, z, (c + dc) % 2)

    for s in NEAR + WHOLE:
        pl.semaphore_signal(barrier, inc=1, device_id=at(0, 0, s), device_id_type=MESH)
    for to in across:
        pl.semaphore_signal(barrier, inc=1, device_id=other(*to), device_id_type=MESH)
    iota_ref[...] = lax.broadcasted_iota(jnp.int32, (256, 128), 0)
    hit_ref[...] = jnp.zeros_like(hit_ref)
    acc_ref[...] = jnp.zeros_like(acc_ref)
    for load in loads[:2]:
        load.wait()
    spread = jnp.concatenate([ids_in[...]] * 8, axis=1).astype(jnp.float32)
    lane = lax.broadcasted_iota(jnp.int32, (1, 128), 1)
    ids_z[0] = jnp.where(lane // 16 == z % 8, spread, 0.0)
    pl.semaphore_wait(barrier, len(NEAR) + len(WHOLE) + len(across))

    def slot(s):
        return (s, x, y) if 8 <= s < 14 else (s, y, x)

    def via(s):
        return 0 if s not in FAR else (12 if s == 9 else 4)

    def ids_copy(s):
        mark = 0 if s == 4 else (1 if s == 12 else 2)
        return send(ids_z.at[via(s)], ids_z.at[s], si, ri.at[mark], at(0, 0, s - via(s)))

    def stage1(s):
        return send(grid.at[slot(via(s))], grid.at[slot(s)], s1, r1.at[s], at(0, 0, s - via(s)))

    def stage2(s, d):
        block = grid.at[slot(s)]
        return send(block, block, s2, r2.at[s], at(d, 0, 0) if s < 8 else at(0, d, 0))

    def stage3(s, d):
        blocks = grid.at[slot(s)[:2]]
        return send(blocks, blocks, s3, r3.at[s], at(0, d, 0) if s < 8 else at(d, 0, 0))

    def mark_whole(s):
        return jnp.where(s < 8, s - 1, 17 - s)

    def sized(ref, out_sem, in_sem):
        return send(ref, ref, out_sem, in_sem, partner)

    def whole(s):
        return send(grid.at[0], grid.at[s], sw, rw.at[mark_whole(s)], at(0, 0, s))

    def export(s):
        return send(grid.at[s], pool_hbm.at[c, s], se, re, partner)

    def export_here(s):
        return pltpu.make_async_copy(grid.at[s], pool_hbm.at[c, s], le)

    own_row = c * 16 + y * 4 + x

    def table_copy(dx, dy, dc):
        dst = table_ref.at[own_row]
        return send(ids_own, dst, st, rt, other(dx, dy, dc))

    swaps = [
        send(users.at[c], users.at[c], su.at[0], ru.at[0], partner),
        send(pos.at[c], pos.at[c], su.at[1], ru.at[1], partner),
    ]
    for s in NEAR:
        ids_copy(s).start()
        stage1(s).start()
    for s in WHOLE:
        ids_copy(s).start()
    for d in (1, 3, 2):
        stage2(0, d).start()
    for load in loads[2:]:
        load.wait()
    for swap in swaps:
        swap.start()

    def turn_users():
        for swap in swaps:
            swap.wait_recv()
        for half in range(2):
            for i in range(4):
                ut[:, pl.ds(half * 1024 + i * 256, 256)] = users[half, pl.ds(i * 256, 256), :].T
        for half in range(2):
            px, py, pz, pc, pe = split(pos[half])
            s = (z - pz + 16) & 15
            block = jnp.where(turned(s) == 0, py * 4 + px, px * 4 + py)
            key_ref[half] = jnp.where(pc == c, s * 256 + block * 16 + pe, -1)

    def share_ids():
        sized(ids_z.at[pl.ds(0, 13)], si, ri.at[2]).wait_recv()
        rows = ids_z[:, 0, :]
        source = (z - lax.broadcasted_iota(jnp.int32, (16, 128), 0) + 16) & 15
        for half in range(2):
            mine = jnp.sum(jnp.where(source // 8 == half, rows, 0.0), axis=0, keepdims=True)
            ids_own[pl.ds(half, 1), :] = mine
        table_ref[own_row] = ids_own[...]
        for to in across:
            table_copy(*to).start()

    def find_ids():
        sized(table_ref.at[pl.ds(0, 31)], st, rt).wait_recv()
        for half in range(2):
            for g in range(8):
                px, py, pz, pc, pe = split(pos[half, pl.ds(g, 1), :])
                pid_ref[half, pl.ds(g, 1), :] = look_up(table_ref, pz * 16 + pe, pc * 16 + py * 4 + px)
        for order in range(2):
            cols_ref[order] = id_columns(table_ref, c, order == 1)

    def evaluate(s):
        block = grid[s].reshape(256, 256)
        for tile in range(8):
            d = jnp.dot(block, ut[:, pl.ds(tile * 256, 256)], preferred_element_type=jnp.float32)
            groups = (tile * 2, tile * 2 + 1)
            wants = [jnp.broadcast_to(key_ref[g // 8, pl.ds(g % 8, 1), :] - s * 256, (8, 128)) for g in groups]
            chosen = [hit_ref[:, pl.ds(g * 128, 128)] for g in groups]
            for k in range(32):
                row = iota_ref[pl.ds(k * 8, 8), :]
                for part in range(2):
                    here = d[k * 8 : k * 8 + 8, part * 128 : part * 128 + 128]
                    prob[s, pl.ds(k * 8, 8), pl.ds(groups[part] * 128, 128)] = jnp.exp2(here * SCALE)
                    chosen[part] = jnp.where(row == wants[part], here, chosen[part])
            for part in range(2):
                hit_ref[:, pl.ds(groups[part] * 128, 128)] = chosen[part]

    def finish_slots(slots):
        for n, s in enumerate(slots):
            fill_ids(idc_ref.at[n], cols_ref, (z - s + 16) & 15, turned(s))
        for n, s in enumerate(slots):
            block = grid[s].reshape(256, 256)
            for tile in range(8):
                d = jnp.dot(block, ut[:, pl.ds(tile * 256, 256)], preferred_element_type=jnp.float32)
                groups = (tile * 2, tile * 2 + 1)
                wants = [jnp.broadcast_to(key_ref[g // 8, pl.ds(g % 8, 1), :] - s * 256, (8, 128)) for g in groups]
                pids = [jnp.broadcast_to(pid_ref[g // 8, pl.ds(g % 8, 1), :], (8, 128)) for g in groups]
                chosen = [hit_ref[:, pl.ds(g * 128, 128)] for g in groups]
                sums = [[acc_ref[:, pl.ds(g * 128, 128)], None] for g in groups]
                for k in range(32):
                    row = iota_ref[pl.ds(k * 8, 8), :]
                    ids = idc_ref[n, pl.ds(k * 8, 8), :]
                    for part in range(2):
                        here = d[k * 8 : k * 8 + 8, part * 128 : part * 128 + 128]
                        term = jnp.where(ids == pids[part], 0.0, jnp.exp2(here * SCALE))
                        old = sums[part][k % 2]
                        sums[part][k % 2] = term if old is None else old + term
                        chosen[part] = jnp.where(row == wants[part], here, chosen[part])
                for part in range(2):
                    lanes = pl.ds(groups[part] * 128, 128)
                    hit_ref[:, lanes] = chosen[part]
                    acc_ref[:, lanes] = sums[part][0] + sums[part][1]

    def collect(s):
        fill_ids(idc_ref.at[0], cols_ref, (z - s + 16) & 15, turned(s))
        for four in range(4):
            groups = [four * 4 + n for n in range(4)]
            pids = [jnp.broadcast_to(pid_ref[g // 8, pl.ds(g % 8, 1), :], (8, 128)) for g in groups]
            sums = [[acc_ref[:, pl.ds(g * 128, 128)], None] for g in groups]
            for k in range(32):
                rows = pl.ds(k * 8, 8)
                ids = idc_ref[0, rows, :]
                for n, g in enumerate(groups):
                    term = jnp.where(ids == pids[n], 0.0, prob[s, rows, pl.ds(g * 128, 128)])
                    sums[n][k % 2] = term if sums[n][k % 2] is None else sums[n][k % 2] + term
            for n, g in enumerate(groups):
                acc_ref[:, pl.ds(g * 128, 128)] = sums[n][0] + sums[n][1]

    def forward(slots):
        for s in slots:
            sized(grid.at[s, 0, pl.ds(0, 3)], s2, r2.at[s]).wait_recv()
            for d in (1, 3, 2):
                stage3(s, d).start()

    def landed(s):
        sized(grid.at[s, pl.ds(0, 3)], s3, r3.at[s]).wait_recv()

    def hand_on(s):
        export(s).start()
        export_here(s).start()

    def loop(first, stop, slot_of, step):
        def turn(i, carry):
            step(slot_of(i))
            return carry

        lax.fori_loop(first, stop, turn, 0)

    def early(slots):
        for s in slots:
            landed(s)
            hand_on(s)
        for s in slots:
            evaluate(s)

    def late_whole(slots):
        for s in slots:
            sized(grid.at[s], sw, rw.at[mark_whole(s)]).wait_recv()
            hand_on(s)
        finish_slots(slots)

    def late(slots):
        for s in slots:
            landed(s)
            hand_on(s)
        finish_slots(slots)

    def take(slots):
        for s in slots:
            stage1(s).wait_recv()
            for d in (1, 3, 2):
                stage2(s, d).start()

    turn_users()
    forward((0,))
    for s in (4, 12):
        ids_copy(s).wait_recv()
        stage1(s).wait_recv()
    for s in FAR:
        ids_copy(s).start()
        stage1(s).start()
    for s in (4, 12):
        for d in (1, 3, 2):
            stage2(s, d).start()
    take((3, 13))
    landed(0)
    for s in WHOLE:
        whole(s).start()
    hand_on(0)
    take((5, 11, 6, 10))
    evaluate(0)
    forward((4, 12, 3, 13))
    share_ids()
    take(FAR)
    early((4, 12))
    forward((5, 11, 6, 10))
    early((3, 13))
    forward(FAR)
    find_ids()
    loop(0, 5, lambda i: jnp.where(i < 2, i * 4, jnp.where(i == 2, 12, 10 * i - 27)), collect)
    loop(0, 2, lambda i: (1 + i, 15 - i), late_whole)
    loop(0, 3, lambda i: (5 + i, 11 - i), late)
    late((8,))

    for half in range(2):
        for g in range(8):
            lanes = pl.ds((half * 8 + g) * 128, 128)
            mine_ref[half, 0, pl.ds(g, 1), :] = jnp.sum(acc_ref[:, lanes], axis=0, keepdims=True)
            mine_ref[half, 1, pl.ds(g, 1), :] = jnp.sum(hit_ref[:, lanes], axis=0, keepdims=True)
    last = send(mine_ref.at[1 - c], theirs_ref, sf, rf, partner)
    last.start()
    for swap in swaps:
        swap.wait_send()
    sized(ids_z.at[pl.ds(0, 15)], si, ri.at[2]).wait_send()
    sized(grid.at[pl.ds(0, 11), 0, 0], s1, r1.at[3]).wait_send()
    sized(grid.at[pl.ds(0, 9), 0], s2, r2.at[0]).wait_send()
    sized(grid.at[pl.ds(0, 9)], s3, r3.at[0]).wait_send()
    sized(grid.at[pl.ds(0, 4)], sw, rw.at[0]).wait_send()
    sized(table_ref.at[pl.ds(0, 31)], st, rt).wait_send()
    send(grid, pool_hbm.at[c], se, re, partner).wait()
    pltpu.make_async_copy(grid, pool_hbm.at[c], le).wait()
    last.wait()
    chosen = mine_ref[c, 1] + theirs_ref[1]
    others = mine_ref[c, 0] + theirs_ref[0]
    own = jnp.exp2(chosen * SCALE)
    total = others + own
    stat_ref[0] = jnp.where(others < own, jnp.log(1.0 + others / own), jnp.log(total) - 0.125 * chosen)
    stat_ref[1] = total
    stat_ref[2] = chosen
    stat_ref[3] = pid_ref[c]


def finish_kernel(stat_ref, table_hbm, users_hbm, pool_hbm, out_ref, table, users, ut, block, cols, idc, high_ref, sum_ref, sem):
    total = stat_ref[1]
    out_ref[...] = stat_ref[0]
    fine = jnp.where((total > SMALL) & (total < LARGE), 0.0, 1.0)

    @pl.when(jnp.max(fine) > 0.0)
    def _():
        z = lax.axis_index("col") // 2
        for src, dst in ((table_hbm, table), (users_hbm, users)):
            copy = pltpu.make_async_copy(src, dst, sem)
            copy.start()
            copy.wait()
        for i in range(4):
            ut[:, pl.ds(i * 256, 256)] = users[pl.ds(i * 256, 256), :].T
        high_ref[...] = jnp.full_like(high_ref, START)
        sum_ref[...] = jnp.zeros_like(sum_ref)
        for core in range(2):
            for order in range(2):
                cols[order] = id_columns(table, core, order == 1)

            def absorb(s, _):
                copy = pltpu.make_async_copy(pool_hbm.at[core, s], block, sem)
                copy.start()
                copy.wait()
                fill_ids(idc, cols, (z - s + 16) & 15, turned(s))
                for g in range(8):
                    lanes = pl.ds(g * 128, 128)
                    d = jnp.dot(block[...].reshape(256, 256), ut[:, lanes], preferred_element_type=jnp.float32)
                    masked = jnp.where(idc[...] == stat_ref[3, pl.ds(g, 1), :], LOW, d * SCALE)
                    high = high_ref[pl.ds(g, 1), :]
                    top = jnp.maximum(high, jnp.max(masked, axis=0, keepdims=True))
                    part = jnp.sum(jnp.exp2(masked - top), axis=0, keepdims=True)
                    sum_ref[pl.ds(g, 1), :] = sum_ref[pl.ds(g, 1), :] * jnp.exp2(high - top) + part
                    high_ref[pl.ds(g, 1), :] = top

                return 0

            lax.fori_loop(0, 16, absorb, 0)
        own = stat_ref[2] * SCALE
        high = high_ref[...]
        top = jnp.maximum(high, own)
        both = sum_ref[...] * jnp.exp2(high - top) + jnp.exp2(own - top)
        out_ref[...] = (top - own) * LN2 + jnp.log(both)


def body(users, positives, items, item_ids):
    hbm = pl.BlockSpec(memory_space=pltpu.HBM)
    vmem = pl.BlockSpec(memory_space=pltpu.VMEM)
    f32, bf16, i32 = jnp.float32, jnp.bfloat16, jnp.int32
    dma = pltpu.SemaphoreType.DMA
    stat, table, pool = pl.pallas_call(
        gather_kernel,
        name="gather_scores",
        out_shape=(
            jax.ShapeDtypeStruct((4, 8, 128), f32),
            jax.ShapeDtypeStruct((32, 2, 128), f32),
            jax.ShapeDtypeStruct((2, 16, 4, 4, 16, 256), bf16),
        ),
        in_specs=[hbm] * 4,
        out_specs=(vmem, vmem, hbm),
        scratch_shapes=[
            pltpu.VMEM((16, 4, 4, 16, 256), bf16),
            pltpu.VMEM((2, 1024, 256), bf16),
            pltpu.VMEM((2, 8, 128), i32),
            pltpu.VMEM((1, 16), i32),
            pltpu.VMEM((16, 1, 128), f32),
            pltpu.VMEM((2, 128), f32),
            pltpu.VMEM((256, 2048), bf16),
            pltpu.VMEM((16, 256, 2048), f32),
            pltpu.VMEM((2, 8, 128), i32),
            pltpu.VMEM((2, 8, 128), f32),
            pltpu.VMEM((256, 128), i32),
            pltpu.VMEM((8, 2048), f32),
            pltpu.VMEM((8, 2048), f32),
            pltpu.VMEM((2, 256, 128), f32),
            pltpu.VMEM((2, 256, 128), f32),
            pltpu.VMEM((2, 2, 8, 128), f32),
            pltpu.VMEM((2, 8, 128), f32),
            dma((4,)),
            dma, dma((14,)),
            dma, dma((14,)),
            dma, dma((14,)),
            dma, dma((4,)),
            dma, dma((3,)),
            dma, dma,
            dma((2,)), dma((2,)),
            dma, dma, dma,
            dma, dma,
        ],
        compiler_params=pltpu.CompilerParams(collective_id=0, has_side_effects=True, vmem_limit_bytes=67_000_000),
    )(users, positives.reshape(8, 128), items, item_ids.reshape(1, 16))
    loss = pl.pallas_call(
        finish_kernel,
        name="finish",
        out_shape=jax.ShapeDtypeStruct((8, 128), f32),
        in_specs=[vmem, hbm, hbm, hbm],
        out_specs=vmem,
        scratch_shapes=[
            pltpu.VMEM((32, 2, 128), f32),
            pltpu.VMEM((1024, 256), bf16),
            pltpu.VMEM((256, 1024), bf16),
            pltpu.VMEM((4, 4, 16, 256), bf16),
            pltpu.VMEM((2, 256, 128), f32),
            pltpu.VMEM((256, 128), f32),
            pltpu.VMEM((8, 128), f32),
            pltpu.VMEM((8, 128), f32),
            dma,
        ],
        compiler_params=pltpu.CompilerParams(vmem_limit_bytes=67_000_000),
    )(stat, table, users, pool)
    return loss.reshape(1024)


def solution(mesh):
    split_all = P(("row", "col"))
    wide = P(("row", "col"), None)
    return jax.shard_map(body, mesh=mesh, in_specs=(wide, split_all, wide, split_all), out_specs=split_all, check_vma=False)
```

```python
import math

import jax
import jax.numpy as jnp
from jax import lax
from jax.experimental import pallas as pl
from jax.experimental.pallas import tpu as pltpu
from jax.sharding import PartitionSpec as P

MESH = pl.DeviceIdType.MESH
SCALE = 0.125 * math.log2(math.e)
LN2 = math.log(2.0)
LOW = -1e30
START = -1e20
SMALL = 2.0**-80
LARGE = 2.0**100
NEAR = (4, 12, 3, 13)
FAR = (8, 9, 7, 10, 6, 11, 5)
WHOLE = (1, 15, 2, 14)


def place():
    row, col = lax.axis_index("row"), lax.axis_index("col")
    return (row // 2) % 4, (col % 2) * 2 + row // 8, col // 2, row % 2


def device(x, y, z, c):
    return ((y % 2) * 4 + x) * 2 + c, z * 2 + y // 2


def id_columns(table, core, x_first):
    halves = []
    for half in range(2):
        if x_first:
            picks = [table[core * 16 + (n % 4) * 4 + n // 4, pl.ds(half, 1), :] for n in range(16)]
            rows = jnp.concatenate(picks, axis=0)
        else:
            rows = table[pl.ds(core * 16, 16), half, :]
        square = jnp.concatenate([rows, jnp.zeros((112, 128), jnp.float32)], axis=0)
        halves.append(square.T)
    return jnp.concatenate(halves, axis=0)


def turned(s):
    return jnp.where((s >= 8) & (s < 14), 1, 0)


def fill_ids(into, columns, z_from, order):
    rows = columns[order, pl.ds(pl.multiple_of(z_from * 16, 16), 16), :]
    for block in range(16):
        into[pl.ds(block * 16, 16), :] = jnp.broadcast_to(rows[:, block : block + 1], (16, 128))


def look_up(table, low, high):
    count = low.shape[1]
    found = None
    for half in range(2):
        ints = table[:, half, :].astype(jnp.int32)
        pieces = jnp.concatenate([ints & 127, (ints >> 7) & 127, ints >> 14], axis=0)
        pieces = pieces.astype(jnp.float32).astype(jnp.bfloat16)
        lanes = lax.broadcasted_iota(jnp.int32, (128, count), 0) + half * 128
        one_hot = jnp.where(lanes == low, 1.0, 0.0).astype(jnp.bfloat16)
        part = jnp.dot(pieces, one_hot, preferred_element_type=jnp.float32)
        found = part if found is None else found + part
    value = found[:32] + 128.0 * found[32:64] + 16384.0 * found[64:]
    mine = lax.broadcasted_iota(jnp.int32, (32, count), 0) == high
    return jnp.sum(jnp.where(mine, value, 0.0), axis=0, keepdims=True)


def split(pos):
    row, col = pos >> 9, (pos >> 4) & 31
    return (row >> 1) & 3, (col & 1) * 2 + (row >> 3), col >> 1, row & 1, pos & 15


def gather_kernel(
    users_hbm, pos_hbm, items_hbm, ids_hbm,
    stat_ref, table_ref, pool_hbm,
    grid, users, pos, ids_in, ids_z, ids_own, ut, prob, key_ref, pid_ref, iota_ref, hit_ref, acc_ref, cols_ref, idc_ref, mine_ref, theirs_ref,
    lsem, s1, r1, s2, r2, s3, r3, sw, rw, si, ri, st, rt, su, ru, se, re, le, sf, rf,
):
    x, y, z, c = place()

    def at(dx, dy, dz):
        return device((x + dx) % 4, (y + dy) % 4, (z + dz) % 16, c)

    partner = device(x, y, z, 1 - c)

    def send(src, dst, out_sem, in_sem, to):
        return pltpu.make_async_remote_copy(src, dst, out_sem, in_sem, device_id=to, device_id_type=MESH)

    barrier = pltpu.get_barrier_semaphore()
    loads = [
        pltpu.make_async_copy(items_hbm, grid.at[0, y, x], lsem.at[0]),
        pltpu.make_async_copy(ids_hbm, ids_in, lsem.at[1]),
        pltpu.make_async_copy(users_hbm, users.at[c], lsem.at[2]),
        pltpu.make_async_copy(pos_hbm, pos.at[c], lsem.at[3]),
    ]
    for load in loads:
        load.start()
    across = [(dx, dy, dc) for dx in range(4) for dy in range(4) for dc in range(2) if (dx, dy, dc) != (0, 0, 0)]

    def other(dx, dy, dc):
        return device((x + dx) % 4, (y + dy) % 4, z, (c + dc) % 2)

    for s in NEAR + WHOLE:
        pl.semaphore_signal(barrier, inc=1, device_id=at(0, 0, s), device_id_type=MESH)
    for to in across:
        pl.semaphore_signal(barrier, inc=1, device_id=other(*to), device_id_type=MESH)
    iota_ref[...] = lax.broadcasted_iota(jnp.int32, (256, 128), 0)
    hit_ref[...] = jnp.zeros_like(hit_ref)
    acc_ref[...] = jnp.zeros_like(acc_ref)
    for load in loads[:2]:
        load.wait()
    spread = jnp.concatenate([ids_in[...]] * 8, axis=1).astype(jnp.float32)
    lane = lax.broadcasted_iota(jnp.int32, (1, 128), 1)
    ids_z[0] = jnp.where(lane // 16 == z % 8, spread, 0.0)
    pl.semaphore_wait(barrier, len(NEAR) + len(WHOLE) + len(across))

    def slot(s):
        return (s, x, y) if 8 <= s < 14 else (s, y, x)

    def via(s):
        return 0 if s not in FAR else (12 if s >= 9 else 4)

    def ids_copy(s):
        mark = 0 if s == 4 else (1 if s == 12 else 2)
        return send(ids_z.at[via(s)], ids_z.at[s], si, ri.at[mark], at(0, 0, s - via(s)))

    def stage1(s):
        return send(grid.at[slot(via(s))], grid.at[slot(s)], s1, r1.at[s], at(0, 0, s - via(s)))

    def stage2(s, d):
        block = grid.at[slot(s)]
        return send(block, block, s2, r2.at[s], at(d, 0, 0) if s < 8 else at(0, d, 0))

    def stage3(s, d):
        blocks = grid.at[slot(s)[:2]]
        return send(blocks, blocks, s3, r3.at[s], at(0, d, 0) if s < 8 else at(d, 0, 0))

    def mark_whole(s):
        return jnp.where(s < 8, s - 1, 17 - s)

    def sized(ref, out_sem, in_sem):
        return send(ref, ref, out_sem, in_sem, partner)

    def whole(s):
        return send(grid.at[0], grid.at[s], sw, rw.at[mark_whole(s)], at(0, 0, s))

    def export(s):
        return send(grid.at[s], pool_hbm.at[c, s], se, re, partner)

    def export_here(s):
        return pltpu.make_async_copy(grid.at[s], pool_hbm.at[c, s], le)

    own_row = c * 16 + y * 4 + x

    def table_copy(dx, dy, dc):
        dst = table_ref.at[own_row]
        return send(ids_own, dst, st, rt, other(dx, dy, dc))

    swaps = [
        send(users.at[c], users.at[c], su.at[0], ru.at[0], partner),
        send(pos.at[c], pos.at[c], su.at[1], ru.at[1], partner),
    ]
    for s in NEAR:
        ids_copy(s).start()
        stage1(s).start()
    for s in WHOLE:
        ids_copy(s).start()
    for d in (1, 3, 2):
        stage2(0, d).start()
    for load in loads[2:]:
        load.wait()
    for swap in swaps:
        swap.start()

    def turn_users():
        for swap in swaps:
            swap.wait_recv()
        for half in range(2):
            for i in range(4):
                ut[:, pl.ds(half * 1024 + i * 256, 256)] = users[half, pl.ds(i * 256, 256), :].T
        for half in range(2):
            px, py, pz, pc, pe = split(pos[half])
            s = (z - pz + 16) & 15
            block = jnp.where(turned(s) == 0, py * 4 + px, px * 4 + py)
            key_ref[half] = jnp.where(pc == c, s * 256 + block * 16 + pe, -1)

    def share_ids():
        sized(ids_z.at[pl.ds(0, 13)], si, ri.at[2]).wait_recv()
        rows = ids_z[:, 0, :]
        source = (z - lax.broadcasted_iota(jnp.int32, (16, 128), 0) + 16) & 15
        for half in range(2):
            mine = jnp.sum(jnp.where(source // 8 == half, rows, 0.0), axis=0, keepdims=True)
            ids_own[pl.ds(half, 1), :] = mine
        table_ref[own_row] = ids_own[...]
        for to in across:
            table_copy(*to).start()

    def find_ids():
        sized(table_ref.at[pl.ds(0, 31)], st, rt).wait_recv()
        for half in range(2):
            for g in range(8):
                px, py, pz, pc, pe = split(pos[half, pl.ds(g, 1), :])
                pid_ref[half, pl.ds(g, 1), :] = look_up(table_ref, pz * 16 + pe, pc * 16 + py * 4 + px)
        for order in range(2):
            cols_ref[order] = id_columns(table_ref, c, order == 1)

    def evaluate(s):
        block = grid[s].reshape(256, 256)
        for tile in range(8):
            d = jnp.dot(block, ut[:, pl.ds(tile * 256, 256)], preferred_element_type=jnp.float32)
            groups = (tile * 2, tile * 2 + 1)
            wants = [jnp.broadcast_to(key_ref[g // 8, pl.ds(g % 8, 1), :] - s * 256, (8, 128)) for g in groups]
            chosen = [hit_ref[:, pl.ds(g * 128, 128)] for g in groups]
            for k in range(32):
                row = iota_ref[pl.ds(k * 8, 8), :]
                for part in range(2):
                    here = d[k * 8 : k * 8 + 8, part * 128 : part * 128 + 128]
                    prob[s, pl.ds(k * 8, 8), pl.ds(groups[part] * 128, 128)] = jnp.exp2(here * SCALE)
                    chosen[part] = jnp.where(row == wants[part], here, chosen[part])
            for part in range(2):
                hit_ref[:, pl.ds(groups[part] * 128, 128)] = chosen[part]

    def finish_slots(slots):
        for n, s in enumerate(slots):
            fill_ids(idc_ref.at[n], cols_ref, (z - s + 16) & 15, turned(s))
        for n, s in enumerate(slots):
            block = grid[s].reshape(256, 256)
            for tile in range(8):
                d = jnp.dot(block, ut[:, pl.ds(tile * 256, 256)], preferred_element_type=jnp.float32)
                groups = (tile * 2, tile * 2 + 1)
                wants = [jnp.broadcast_to(key_ref[g // 8, pl.ds(g % 8, 1), :] - s * 256, (8, 128)) for g in groups]
                pids = [jnp.broadcast_to(pid_ref[g // 8, pl.ds(g % 8, 1), :], (8, 128)) for g in groups]
                chosen = [hit_ref[:, pl.ds(g * 128, 128)] for g in groups]
                sums = [[acc_ref[:, pl.ds(g * 128, 128)], None] for g in groups]
                for k in range(32):
                    row = iota_ref[pl.ds(k * 8, 8), :]
                    ids = idc_ref[n, pl.ds(k * 8, 8), :]
                    for part in range(2):
                        here = d[k * 8 : k * 8 + 8, part * 128 : part * 128 + 128]
                        term = jnp.where(ids == pids[part], 0.0, jnp.exp2(here * SCALE))
                        old = sums[part][k % 2]
                        sums[part][k % 2] = term if old is None else old + term
                        chosen[part] = jnp.where(row == wants[part], here, chosen[part])
                for part in range(2):
                    lanes = pl.ds(groups[part] * 128, 128)
                    hit_ref[:, lanes] = chosen[part]
                    acc_ref[:, lanes] = sums[part][0] + sums[part][1]

    def collect(s):
        fill_ids(idc_ref.at[0], cols_ref, (z - s + 16) & 15, turned(s))
        for four in range(4):
            groups = [four * 4 + n for n in range(4)]
            pids = [jnp.broadcast_to(pid_ref[g // 8, pl.ds(g % 8, 1), :], (8, 128)) for g in groups]
            sums = [[acc_ref[:, pl.ds(g * 128, 128)], None] for g in groups]
            for k in range(32):
                rows = pl.ds(k * 8, 8)
                ids = idc_ref[0, rows, :]
                for n, g in enumerate(groups):
                    term = jnp.where(ids == pids[n], 0.0, prob[s, rows, pl.ds(g * 128, 128)])
                    sums[n][k % 2] = term if sums[n][k % 2] is None else sums[n][k % 2] + term
            for n, g in enumerate(groups):
                acc_ref[:, pl.ds(g * 128, 128)] = sums[n][0] + sums[n][1]

    def forward(slots):
        for s in slots:
            sized(grid.at[s, 0, pl.ds(0, 3)], s2, r2.at[s]).wait_recv()
            for d in (1, 3, 2):
                stage3(s, d).start()

    def landed(s):
        sized(grid.at[s, pl.ds(0, 3)], s3, r3.at[s]).wait_recv()

    def hand_on(s):
        export(s).start()
        export_here(s).start()

    def loop(first, stop, slot_of, step):
        def turn(i, carry):
            step(slot_of(i))
            return carry

        lax.fori_loop(first, stop, turn, 0)

    def early(slots):
        for s in slots:
            landed(s)
            hand_on(s)
        for s in slots:
            evaluate(s)

    def late_whole(slots):
        for s in slots:
            sized(grid.at[s], sw, rw.at[mark_whole(s)]).wait_recv()
            hand_on(s)
        finish_slots(slots)

    def late(slots):
        for s in slots:
            landed(s)
            hand_on(s)
        finish_slots(slots)

    def take(slots):
        for s in slots:
            stage1(s).wait_recv()
            for d in (1, 3, 2):
                stage2(s, d).start()

    turn_users()
    forward((0,))
    for s in (4, 12):
        ids_copy(s).wait_recv()
        stage1(s).wait_recv()
    for s in FAR:
        ids_copy(s).start()
        stage1(s).start()
    for s in (4, 12):
        for d in (1, 3, 2):
            stage2(s, d).start()
    take((3, 13))
    landed(0)
    for s in WHOLE:
        whole(s).start()
    hand_on(0)
    evaluate(0)
    forward((4, 12, 3, 13))
    share_ids()
    take(FAR)
    early((4, 12))
    forward(FAR[:4])
    early((3, 13))
    forward(FAR[4:])
    find_ids()
    loop(0, 5, lambda i: jnp.where(i < 2, i * 4, jnp.where(i == 2, 12, 10 * i - 27)), collect)
    loop(0, 2, lambda i: (1 + i, 15 - i), late_whole)
    loop(0, 3, lambda i: (5 + i, 11 - i), late)
    late((8,))

    for half in range(2):
        for g in range(8):
            lanes = pl.ds((half * 8 + g) * 128, 128)
            mine_ref[half, 0, pl.ds(g, 1), :] = jnp.sum(acc_ref[:, lanes], axis=0, keepdims=True)
            mine_ref[half, 1, pl.ds(g, 1), :] = jnp.sum(hit_ref[:, lanes], axis=0, keepdims=True)
    last = send(mine_ref.at[1 - c], theirs_ref, sf, rf, partner)
    last.start()
    for swap in swaps:
        swap.wait_send()
    sized(ids_z.at[pl.ds(0, 15)], si, ri.at[2]).wait_send()
    sized(grid.at[pl.ds(0, 11), 0, 0], s1, r1.at[3]).wait_send()
    sized(grid.at[pl.ds(0, 9), 0], s2, r2.at[0]).wait_send()
    sized(grid.at[pl.ds(0, 9)], s3, r3.at[0]).wait_send()
    sized(grid.at[pl.ds(0, 4)], sw, rw.at[0]).wait_send()
    sized(table_ref.at[pl.ds(0, 31)], st, rt).wait_send()
    send(grid, pool_hbm.at[c], se, re, partner).wait()
    pltpu.make_async_copy(grid, pool_hbm.at[c], le).wait()
    last.wait()
    chosen = mine_ref[c, 1] + theirs_ref[1]
    others = mine_ref[c, 0] + theirs_ref[0]
    own = jnp.exp2(chosen * SCALE)
    total = others + own
    stat_ref[0] = jnp.where(others < own, jnp.log(1.0 + others / own), jnp.log(total) - 0.125 * chosen)
    stat_ref[1] = total
    stat_ref[2] = chosen
    stat_ref[3] = pid_ref[c]


def finish_kernel(stat_ref, table_hbm, users_hbm, pool_hbm, out_ref, table, users, ut, block, cols, idc, high_ref, sum_ref, sem):
    total = stat_ref[1]
    out_ref[...] = stat_ref[0]
    fine = jnp.where((total > SMALL) & (total < LARGE), 0.0, 1.0)

    @pl.when(jnp.max(fine) > 0.0)
    def _():
        z = lax.axis_index("col") // 2
        for src, dst in ((table_hbm, table), (users_hbm, users)):
            copy = pltpu.make_async_copy(src, dst, sem)
            copy.start()
            copy.wait()
        for i in range(4):
            ut[:, pl.ds(i * 256, 256)] = users[pl.ds(i * 256, 256), :].T
        high_ref[...] = jnp.full_like(high_ref, START)
        sum_ref[...] = jnp.zeros_like(sum_ref)
        for core in range(2):
            for order in range(2):
                cols[order] = id_columns(table, core, order == 1)

            def absorb(s, _):
                copy = pltpu.make_async_copy(pool_hbm.at[core, s], block, sem)
                copy.start()
                copy.wait()
                fill_ids(idc, cols, (z - s + 16) & 15, turned(s))
                for g in range(8):
                    lanes = pl.ds(g * 128, 128)
                    d = jnp.dot(block[...].reshape(256, 256), ut[:, lanes], preferred_element_type=jnp.float32)
                    masked = jnp.where(idc[...] == stat_ref[3, pl.ds(g, 1), :], LOW, d * SCALE)
                    high = high_ref[pl.ds(g, 1), :]
                    top = jnp.maximum(high, jnp.max(masked, axis=0, keepdims=True))
                    part = jnp.sum(jnp.exp2(masked - top), axis=0, keepdims=True)
                    sum_ref[pl.ds(g, 1), :] = sum_ref[pl.ds(g, 1), :] * jnp.exp2(high - top) + part
                    high_ref[pl.ds(g, 1), :] = top

                return 0

            lax.fori_loop(0, 16, absorb, 0)
        own = stat_ref[2] * SCALE
        high = high_ref[...]
        top = jnp.maximum(high, own)
        both = sum_ref[...] * jnp.exp2(high - top) + jnp.exp2(own - top)
        out_ref[...] = (top - own) * LN2 + jnp.log(both)


def body(users, positives, items, item_ids):
    hbm = pl.BlockSpec(memory_space=pltpu.HBM)
    vmem = pl.BlockSpec(memory_space=pltpu.VMEM)
    f32, bf16, i32 = jnp.float32, jnp.bfloat16, jnp.int32
    dma = pltpu.SemaphoreType.DMA
    stat, table, pool = pl.pallas_call(
        gather_kernel,
        name="gather_scores",
        out_shape=(
            jax.ShapeDtypeStruct((4, 8, 128), f32),
            jax.ShapeDtypeStruct((32, 2, 128), f32),
            jax.ShapeDtypeStruct((2, 16, 4, 4, 16, 256), bf16),
        ),
        in_specs=[hbm] * 4,
        out_specs=(vmem, vmem, hbm),
        scratch_shapes=[
            pltpu.VMEM((16, 4, 4, 16, 256), bf16),
            pltpu.VMEM((2, 1024, 256), bf16),
            pltpu.VMEM((2, 8, 128), i32),
            pltpu.VMEM((1, 16), i32),
            pltpu.VMEM((16, 1, 128), f32),
            pltpu.VMEM((2, 128), f32),
            pltpu.VMEM((256, 2048), bf16),
            pltpu.VMEM((16, 256, 2048), f32),
            pltpu.VMEM((2, 8, 128), i32),
            pltpu.VMEM((2, 8, 128), f32),
            pltpu.VMEM((256, 128), i32),
            pltpu.VMEM((8, 2048), f32),
            pltpu.VMEM((8, 2048), f32),
            pltpu.VMEM((2, 256, 128), f32),
            pltpu.VMEM((2, 256, 128), f32),
            pltpu.VMEM((2, 2, 8, 128), f32),
            pltpu.VMEM((2, 8, 128), f32),
            dma((4,)),
            dma, dma((14,)),
            dma, dma((14,)),
            dma, dma((14,)),
            dma, dma((4,)),
            dma, dma((3,)),
            dma, dma,
            dma((2,)), dma((2,)),
            dma, dma, dma,
            dma, dma,
        ],
        compiler_params=pltpu.CompilerParams(collective_id=0, has_side_effects=True, vmem_limit_bytes=67_000_000),
    )(users, positives.reshape(8, 128), items, item_ids.reshape(1, 16))
    loss = pl.pallas_call(
        finish_kernel,
        name="finish",
        out_shape=jax.ShapeDtypeStruct((8, 128), f32),
        in_specs=[vmem, hbm, hbm, hbm],
        out_specs=vmem,
        scratch_shapes=[
            pltpu.VMEM((32, 2, 128), f32),
            pltpu.VMEM((1024, 256), bf16),
            pltpu.VMEM((256, 1024), bf16),
            pltpu.VMEM((4, 4, 16, 256), bf16),
            pltpu.VMEM((2, 256, 128), f32),
            pltpu.VMEM((256, 128), f32),
            pltpu.VMEM((8, 128), f32),
            pltpu.VMEM((8, 128), f32),
            dma,
        ],
        compiler_params=pltpu.CompilerParams(vmem_limit_bytes=67_000_000),
    )(stat, table, users, pool)
    return loss.reshape(1024)


def solution(mesh):
    split_all = P(("row", "col"))
    wide = P(("row", "col"), None)
    return jax.shard_map(body, mesh=mesh, in_specs=(wide, split_all, wide, split_all), out_specs=split_all, check_vma=False)
```
